32 devices in a mesh: fsdp: 4 (over y, x), tp: 8 (over z, core).
Axes of the slice: x: 2, y: 2, z: 4, core: 2. Of those that a mesh axis runs over, the one named last changes fastest.
Arguments:
- ref_gate: bfloat16 [3072, 11008], P('fsdp', 'tp'), may hold values from -6 to 6
- ref_up: bfloat16 [3072, 11008], P('fsdp', 'tp'), may hold values from -6 to 6
- ref_residual: bfloat16 [3072, 4096], P('fsdp', 'tp'), may hold values from -6 to 6
- ref_modality: int32 [3072], P('fsdp'), may hold values 0 or 1
- ref_down_text: bfloat16 [4096, 11008], P('fsdp', 'tp'), may hold values from -0.0546875 to 0.0546875
- ref_down_image: bfloat16 [4096, 11008], P('fsdp', 'tp'), may hold values from -0.0546875 to 0.0546875
- pol_gate: bfloat16 [3072, 11008], P('fsdp', 'tp'), may hold values from -6 to 6
- pol_up: bfloat16 [3072, 11008], P('fsdp', 'tp'), may hold values from -6 to 6
- pol_modality: int32 [3072], P('fsdp'), may hold values 0 or 1
- pol_segment: int32 [3072], P('fsdp'), may hold values from 0 to 5, never falling along the last dimension, each value on 1 to 768 neighbouring positions
- pair_margin: float32 [3], replicated, may hold values from -30 to 30
- token_cotangent: bfloat16 [3072, 4096], P('fsdp', 'tp'), may hold values from -24 to 24
- pol_down_text: bfloat16 [4096, 11008], P('fsdp', 'tp'), may hold values from -0.0546875 to 0.0546875
- pol_down_image: bfloat16 [4096, 11008], P('fsdp', 'tp'), may hold values from -0.0546875 to 0.0546875
Outputs:
- ref_out: bfloat16 [3072, 4096], P('fsdp', 'tp')
- grad_gate: bfloat16 [3072, 11008], P('fsdp', 'tp')
- grad_up: bfloat16 [3072, 11008], P('fsdp', 'tp')
- grad_down_text: float32 [4096, 11008], P('fsdp', 'tp')
- grad_down_image: float32 [4096, 11008], P('fsdp', 'tp')
The draws below stay inside these ranges and needn't reach their ends.
Inputs may be any that keep to these rules, and one draw needn't show every extreme that they name: `ref_modality`: 0 marks a text token, 1 an image token. `pol_modality`: 0 marks a text token, 1 an image token. `pol_segment`: response numbers never fall along the tokens; responses 2p and 2p + 1 are the chosen and the rejected response of pair p; every response has at least one token.
All inputs are finite; a program needn't handle non-finite values. No bound on the sum of `ref_modality` or of `pol_modality` on one device may be relied on, other than what follows from the above.
Results may differ from the reference program's by a relative error of at most 0.015.
Values may be sent and summed in bfloat16 or wider, within the bound.
A program may use at most 192 MiB of HBM per device.

```python
import math
import jax
import jax.numpy as jnp
import numpy as np
from jax import lax

D = 4096
FF = 11008
SEQ = 512
TOKENS = 3072
PAIRS = 3
N_FSDP = 4
N_TP = 8


def plant(entries, rng, smallest, top_value):
    longest = entries.shape.index(max(entries.shape))
    spots = []
    for shift in (0, 1):
        where = [jax.random.randint(jax.random.fold_in(rng, axis), (), 0, length) for axis, length in enumerate(entries.shape)]
        where[longest] = (where[longest] + shift) % entries.shape[longest]
        spots.append(tuple(where))
    return entries.at[spots[0]].set(smallest).at[spots[1]].set(top_value)


def block_levels(own_key, dims, pieces, least, largest):
    def one(position, shards_of):
        steps = jax.random.uniform(jax.random.fold_in(jax.random.fold_in(own_key, 6), position), (shards_of,), jnp.float32, least / len(pieces), largest / len(pieces))
        return jnp.repeat(jnp.exp(steps), dims[position] // shards_of).reshape((-1,) + (1,) * (len(dims) - position - 1))

    factor_of = one(*pieces[0])
    for cut in pieces[1:]:
        factor_of = factor_of * one(*cut)
    return factor_of


def profile(number_of, total, bound, slope):
    weights = [(1 << 20) // math.isqrt(standing ** slope) + 1 for standing in range(2, number_of + 1)]
    spare, counts = total - bound - (number_of - 1), [1] * (number_of - 1)
    while spare > 0:
        movable = [i for i in range(number_of - 1) if counts[i] < bound]
        whole, left = sum([weights[i] for i in movable]), spare
        for i in movable:
            extra = min(bound - counts[i], max(1, left * weights[i] // whole), spare)
            counts[i] = counts[i] + extra
            spare = spare - extra
    return np.array([bound] + counts)


def ragged_sizes(own_key, amount, total, bound, lean):
    if amount == 2:
        one = jax.random.randint(own_key, (), max(1, total - bound), min(bound, total - 1) + 1)
        return jnp.stack([one, total - one])
    lengths = jnp.asarray(profile(amount, total, bound, lean), jnp.int32)
    twos = (amount - 1) // 2
    source_of, receiver = lengths[1:1 + 2 * twos:2], lengths[2:2 + 2 * twos:2]
    margin = jnp.minimum(source_of - 1, bound - receiver)
    shifted = jax.random.randint(jax.random.fold_in(own_key, 1), (twos,), 0, 1 << 20) % (margin + 1)
    lengths = lengths.at[1:1 + 2 * twos:2].set(source_of - shifted).at[2:2 + 2 * twos:2].set(receiver + shifted)
    return lengths[jax.random.permutation(jax.random.fold_in(own_key, 2), amount)]


def normal_values(rng, dims, deviation, limit, pieces=(), held_as=jnp.bfloat16):
    factor_of = block_levels(rng, dims, pieces, -0.22, 0.18) if pieces else 1.0
    result = jax.random.normal(rng, dims, jnp.float32) * deviation * factor_of
    return jnp.minimum(jnp.maximum(result, -limit), limit).astype(held_as)


def setup_inputs(seed: int = 0) -> dict:
    seeds = jax.random.split(jax.random.key(seed), 15)
    ref_gate = normal_values(seeds[0], (TOKENS, FF), 1.0, 6.0, ((0, 4), (1, 8)))
    ref_up = normal_values(seeds[1], (TOKENS, FF), 1.0, 6.0, ((0, 4), (1, 8)))
    ref_residual = normal_values(seeds[2], (TOKENS, D), 1.0, 6.0, ((0, 4), (1, 8)))
    ref_modality = plant((jax.random.randint(seeds[3], (TOKENS,), 0, 5) < 2).astype(jnp.int32), jax.random.fold_in(seeds[3], 1), 0, 1)
    ref_down_text = normal_values(seeds[4], (D, FF), FF ** -0.5, 0.0546875, ((0, 4), (1, 8)))
    ref_down_image = normal_values(seeds[5], (D, FF), FF ** -0.5, 0.0546875, ((0, 4), (1, 8)))
    pol_gate = normal_values(seeds[6], (TOKENS, FF), 1.0, 6.0, ((0, 4), (1, 8)))
    pol_up = normal_values(seeds[7], (TOKENS, FF), 1.0, 6.0, ((0, 4), (1, 8)))
    pol_modality = plant((jax.random.randint(seeds[8], (TOKENS,), 0, 5) < 2).astype(jnp.int32), jax.random.fold_in(seeds[8], 1), 0, 1)
    pol_segment = jnp.searchsorted(jnp.cumsum(ragged_sizes(seeds[9], 2 * PAIRS, TOKENS, SEQ + SEQ // 2, 0)), jnp.arange(TOKENS), side="right").astype(jnp.int32)
    pair_margin = jnp.clip(jax.random.uniform(seeds[10], (PAIRS,), jnp.float32, -30.0, 30.0), -30.0, 30.0)
    token_cotangent = normal_values(seeds[11], (TOKENS, D), 4.0, 24.0, ((0, 4), (1, 8)))
    pol_down_text = normal_values(seeds[12], (D, FF), FF ** -0.5, 0.0546875, ((0, 4), (1, 8)))
    pol_down_image = normal_values(seeds[13], (D, FF), FF ** -0.5, 0.0546875, ((0, 4), (1, 8)))
    return {"ref_gate": ref_gate, "ref_up": ref_up, "ref_residual": ref_residual, "ref_modality": ref_modality, "ref_down_text": ref_down_text, "ref_down_image": ref_down_image, "pol_gate": pol_gate, "pol_up": pol_up, "pol_modality": pol_modality, "pol_segment": pol_segment, "pair_margin": pair_margin, "token_cotangent": token_cotangent, "pol_down_text": pol_down_text, "pol_down_image": pol_down_image}


dpo_beta = 0.1


def split_hidden(gate, up, modality):
    gate_f = gate.astype(jnp.float32)
    up_f = up.astype(jnp.float32)
    sig = jax.nn.sigmoid(gate_f)
    act = gate_f * sig
    hidden = (act * up_f).astype(jnp.bfloat16)
    image = (modality == 1)[:, None]
    zero = jnp.zeros_like(hidden)
    return jnp.where(image, zero, hidden), jnp.where(image, hidden, zero), gate_f, up_f, sig, act


def reference(ref_gate, ref_up, ref_residual, ref_modality, ref_down_text, ref_down_image, pol_gate, pol_up, pol_modality, pol_segment, pair_margin, token_cotangent, pol_down_text, pol_down_image):
    ref_text, ref_image, _, _, _, _ = split_hidden(ref_gate, ref_up, ref_modality)
    block_width = FF // N_TP
    contract = (((1,), (1,)), ((), ()))

    def ref_block(index, total):
        start = (index * block_width).astype(jnp.int32)
        left_text = lax.dynamic_slice_in_dim(ref_text, start, block_width, 1)
        left_image = lax.dynamic_slice_in_dim(ref_image, start, block_width, 1)
        right_text = lax.dynamic_slice_in_dim(ref_down_text, start, block_width, 1)
        right_image = lax.dynamic_slice_in_dim(ref_down_image, start, block_width, 1)
        part = lax.dot_general(left_text, right_text, contract, preferred_element_type=jnp.float32)
        part = part + lax.dot_general(left_image, right_image, contract, preferred_element_type=jnp.float32)
        rounded = lax.optimization_barrier(part.astype(jnp.bfloat16))
        return total + rounded.astype(jnp.float32)

    summed = lax.fori_loop(0, N_TP, ref_block, jnp.zeros((TOKENS, D), jnp.float32))
    ref_out = (summed + ref_residual.astype(jnp.float32)).astype(jnp.bfloat16)

    pol_text, pol_image, gate_f, up_f, sig, act = split_hidden(pol_gate, pol_up, pol_modality)
    seg_ids = jnp.arange(2 * PAIRS, dtype=jnp.int32)
    pair_weight = dpo_beta * jax.nn.sigmoid(-dpo_beta * pair_margin)
    table = jnp.repeat(pair_weight, 2) * jnp.where(seg_ids % 2 == 0, -1.0, 1.0).astype(jnp.float32)
    coef = jnp.sum(jnp.where(pol_segment[:, None] == seg_ids[None, :], table[None, :], jnp.float32(0.0)), axis=1)
    cot = (coef[:, None] * token_cotangent.astype(jnp.float32)).astype(jnp.bfloat16)
    image_p = (pol_modality == 1)[:, None]
    zero_cot = jnp.zeros_like(cot)
    cot_text = jnp.where(image_p, zero_cot, cot)
    cot_image = jnp.where(image_p, cot, zero_cot)
    d_hidden = jnp.dot(cot_text, pol_down_text, preferred_element_type=jnp.float32)
    d_hidden = d_hidden + jnp.dot(cot_image, pol_down_image, preferred_element_type=jnp.float32)
    grad_gate = (d_hidden * up_f * sig * (1.0 + gate_f * (1.0 - sig))).astype(jnp.bfloat16)
    grad_up = (d_hidden * act).astype(jnp.bfloat16)

    rows_block = TOKENS // N_FSDP
    over_rows = (((0,), (0,)), ((), ()))

    def grad_block(index, totals):
        start = (index * rows_block).astype(jnp.int32)
        y_text = lax.dynamic_slice_in_dim(cot_text, start, rows_block, 0)
        y_image = lax.dynamic_slice_in_dim(cot_image, start, rows_block, 0)
        h_text = lax.dynamic_slice_in_dim(pol_text, start, rows_block, 0)
        h_image = lax.dynamic_slice_in_dim(pol_image, start, rows_block, 0)
        term_text = lax.dot_general(y_text, h_text, over_rows, preferred_element_type=jnp.float32)
        term_image = lax.dot_general(y_image, h_image, over_rows, preferred_element_type=jnp.float32)
        term_text = lax.optimization_barrier(term_text.astype(jnp.bfloat16)).astype(jnp.float32)
        term_image = lax.optimization_barrier(term_image.astype(jnp.bfloat16)).astype(jnp.float32)
        return (totals[0] + term_text, totals[1] + term_image)

    start_grads = (jnp.zeros((D, FF), jnp.float32), jnp.zeros((D, FF), jnp.float32))
    grad_down_text, grad_down_image = lax.fori_loop(0, N_FSDP, grad_block, start_grads)
    return (ref_out, grad_gate, grad_up, grad_down_text, grad_down_image)
```

```python
import jax
import jax.numpy as jnp
from jax import lax
from jax.sharding import PartitionSpec as P


dpo_beta = 0.1


def silu_parts(gate, up):
    gate_f = gate.astype(jnp.float32)
    up_f = up.astype(jnp.float32)
    sig = jax.nn.sigmoid(gate_f)
    act = gate_f * sig
    return gate_f, up_f, sig, act


def hidden_of(gate, up):
    _, up_f, _, act = silu_parts(gate, up)
    return (act * up_f).astype(jnp.bfloat16)


def swap_pairs(n_fsdp, n_tp):
    r = n_tp // n_fsdp
    return [
        (f * n_tp + q * r + j, q * n_tp + f * r + j)
        for f in range(n_fsdp)
        for q in range(n_fsdp)
        for j in range(r)
    ]


def gather_modality(ref_modality, pol_modality, n_fsdp):
    own = jnp.stack([ref_modality, pol_modality])
    me = lax.axis_index("fsdp")
    both = jnp.zeros((n_fsdp,) + own.shape, own.dtype)
    both = lax.dynamic_update_index_in_dim(both, own, me, 0)
    for s in range(1, n_fsdp):
        got = lax.ppermute(own, "fsdp", [(i, (i + s) % n_fsdp) for i in range(n_fsdp)])
        both = lax.dynamic_update_index_in_dim(both, got, (me - s) % n_fsdp, 0)
    return both[:, 0].reshape(-1), both[:, 1].reshape(-1)


def per_device(
    n_fsdp,
    n_tp,
    ref_gate,
    ref_up,
    ref_residual,
    ref_modality,
    ref_down_text,
    ref_down_image,
    pol_gate,
    pol_up,
    pol_modality,
    pol_segment,
    pair_margin,
    token_cotangent,
    pol_down_text,
    pol_down_image,
):
    rows, feats = token_cotangent.shape
    pairs = swap_pairs(n_fsdp, n_tp)
    partner = [(t, t ^ 1) for t in range(n_tp)]
    index = lax.axis_index("tp")
    line, half = index // 2, index % 2

    def shift(step):
        return [(t, (t + 2 * step) % n_tp) for t in range(n_tp)]

    seg_ids = jnp.arange(2 * pair_margin.shape[0], dtype=jnp.int32)
    pair_weight = dpo_beta * jax.nn.sigmoid(-dpo_beta * pair_margin)
    table = jnp.repeat(pair_weight, 2) * jnp.where(seg_ids % 2 == 0, -1.0, 1.0).astype(jnp.float32)
    coef = jnp.sum(
        jnp.where(pol_segment[:, None] == seg_ids[None, :], table[None, :], jnp.float32(0.0)),
        axis=1,
    )
    pol_own = hidden_of(pol_gate, pol_up)
    pol_hidden = lax.all_gather(pol_own, "fsdp", axis=0, tiled=True)
    ref_own = hidden_of(ref_gate, ref_up)
    ref_hidden = lax.all_gather(ref_own, "fsdp", axis=0, tiled=True)

    local_cot = (coef[:, None] * token_cotangent.astype(jnp.float32)).astype(jnp.bfloat16)
    moved = lax.ppermute(local_cot, ("fsdp", "tp"), pairs)
    modality_r, modality_p = gather_modality(ref_modality, pol_modality, n_fsdp)
    image_r = (modality_r == 1)[:, None]
    image_p = (modality_p == 1)[:, None]

    mine = jnp.zeros((n_fsdp, rows, feats), jnp.bfloat16)
    mine = lax.dynamic_update_index_in_dim(mine, moved, line, 0)
    for s in range(1, n_fsdp):
        got = lax.ppermute(moved, "tp", shift(s))
        mine = lax.dynamic_update_index_in_dim(mine, got, (line - s) % n_fsdp, 0)
    mine = mine.reshape(n_fsdp * rows, feats)
    theirs = lax.ppermute(mine, "tp", partner)
    first = half == 0
    cot_full = jnp.concatenate(
        [jnp.where(first, mine, theirs), jnp.where(first, theirs, mine)], axis=1
    )

    dh_text = jnp.dot(cot_full, pol_down_text, preferred_element_type=jnp.float32)
    dh_image = jnp.dot(cot_full, pol_down_image, preferred_element_type=jnp.float32)
    dh_part = jnp.where(image_p, dh_image, dh_text).astype(jnp.bfloat16)
    d_hidden = lax.psum_scatter(dh_part, "fsdp", scatter_dimension=0, tiled=True)

    zero = jnp.zeros_like(cot_full)
    over_rows = (((0,), (0,)), ((), ()))
    g_text = lax.dot_general(
        jnp.where(image_p, zero, cot_full), pol_hidden, over_rows, preferred_element_type=jnp.float32
    )
    g_image = lax.dot_general(
        jnp.where(image_p, cot_full, zero), pol_hidden, over_rows, preferred_element_type=jnp.float32
    )

    contract = (((1,), (1,)), ((), ()))

    def out_half(which):
        w_text = lax.dynamic_slice_in_dim(ref_down_text, which * feats, feats, 0)
        w_image = lax.dynamic_slice_in_dim(ref_down_image, which * feats, feats, 0)
        o_text = lax.dot_general(ref_hidden, w_text, contract, preferred_element_type=jnp.float32)
        o_image = lax.dot_general(ref_hidden, w_image, contract, preferred_element_type=jnp.float32)
        return jnp.where(image_r, o_image, o_text).astype(jnp.bfloat16)

    got = lax.ppermute(out_half(1 - half), "tp", partner)
    keep = out_half(half)
    both = (keep.astype(jnp.float32) + got.astype(jnp.float32)).astype(jnp.bfloat16)
    both = both.reshape(n_fsdp, rows, feats)
    total = lax.dynamic_index_in_dim(both, line, 0, keepdims=False).astype(jnp.float32)
    for s in range(1, n_fsdp):
        piece = lax.dynamic_index_in_dim(both, (line + s) % n_fsdp, 0, keepdims=False)
        total = total + lax.ppermute(piece, "tp", shift(s)).astype(jnp.float32)
    summed = lax.ppermute(total.astype(jnp.bfloat16), ("fsdp", "tp"), pairs)
    ref_out = (summed.astype(jnp.float32) + ref_residual.astype(jnp.float32)).astype(jnp.bfloat16)

    late_gate, late_up, d_hidden = lax.optimization_barrier((pol_gate, pol_up, d_hidden))
    gate_f, up_f, sig, act = silu_parts(late_gate, late_up)
    d_hidden = d_hidden.astype(jnp.float32)
    grad_gate = (d_hidden * up_f * sig * (1.0 + gate_f * (1.0 - sig))).astype(jnp.bfloat16)
    grad_up = (d_hidden * act).astype(jnp.bfloat16)
    return (ref_out, grad_gate, grad_up, g_text, g_image)


def solution(mesh):
    n_fsdp, n_tp = mesh.shape["fsdp"], mesh.shape["tp"]
    two = P("fsdp", "tp")
    one = P("fsdp")
    in_specs = (two, two, two, one, two, two, two, two, one, one, P(), two, two, two)

    def body(*args):
        return per_device(n_fsdp, n_tp, *args)

    return jax.shard_map(
        body, mesh=mesh, in_specs=in_specs, out_specs=(two,) * 5, check_vma=False
    )
```
